128 devices in a mesh: rows: 16 (over z, y), cols: 8 (over x, core).
Axes of the slice: x: 4, y: 4, z: 4, core: 2. Of those that a mesh axis runs over, the one named last changes fastest.
Arguments:
- grad_stack: float32 [512, 64, 2048], P(None, 'rows', 'cols'), may hold values from -6 to 6
- moment_stack: float32 [512, 64, 2048], P(None, 'rows', 'cols'), may hold values from -6 to 6
- weight_stack: float32 [512, 64, 2048], P(None, 'rows', 'cols'), may hold values from -0.1875 to 0.1875
Outputs:
- new_weights: float32 [512, 64, 2048], P(None, 'rows', 'cols')
- new_momentum: float32 [512, 64, 2048], P(None, 'rows', 'cols')
The draws below stay inside these ranges and needn't reach their ends.
All inputs are finite; a program needn't handle non-finite values.
Results may differ from the reference program's by a relative error of at most 0.0003.
Values sent between devices are 32-bit elements.
A program may use at most 128 MiB of HBM per device.

```python
import jax
import jax.numpy as jnp
from jax import lax

SIDE = 64
WIDE = 2048
MATS = 512
ITERS = 5


def block_levels(rng, extent, shards, least, high):
    loudness, own = 1.0, jax.random.fold_in(rng, 6)
    for axis_at, shards_of in shards:
        steps = jnp.exp(jax.random.uniform(jax.random.fold_in(own, axis_at), (shards_of,), jnp.float32, least / len(shards), high / len(shards)))
        loudness = loudness * jnp.repeat(steps, extent[axis_at] // shards_of).reshape([-1 if axis == axis_at else 1 for axis in range(len(extent))])
    return loudness


def centred(own_key, dims, spread, most, cuts=(), dtype=jnp.bfloat16):
    loudness = block_levels(own_key, dims, cuts, -0.22, 0.18) if cuts else 1.0
    array = jax.random.normal(own_key, dims, jnp.float32) * spread * loudness
    return jnp.minimum(jnp.maximum(array, -most), most).astype(dtype)


def setup_inputs(seed: int = 0) -> dict:
    key_list = jax.random.split(jax.random.key(seed), 4)
    return {
        "grad_stack": centred(key_list[0], (MATS, SIDE, WIDE), 1.0, 6.0, ((1, 16), (2, 8)), jnp.float32),
        "moment_stack": centred(key_list[1], (MATS, SIDE, WIDE), 1.0, 6.0, ((1, 16), (2, 8)), jnp.float32),
        "weight_stack": centred(key_list[2], (MATS, SIDE, WIDE), 0.03, 0.1875, ((1, 16), (2, 8)), jnp.float32),
    }


hold_rate = 0.95
learn_rate = 1.0

def reference(grad_stack, moment_stack, weight_stack):
    new_momentum = hold_rate * moment_stack + grad_stack

    def orthogonal_one(stack):
        iterate = stack[None]
        iterate = iterate * lax.rsqrt(lax.optimization_barrier(jnp.sum(iterate * iterate, axis=(1, 2), keepdims=True)) + 1e-06)
        for step in range(ITERS):
            gram = jnp.einsum('mik,mjk->mij', iterate, iterate, precision=lax.Precision.HIGHEST)
            mixed = -4.775 * gram + 2.0315 * jnp.einsum('mij,mjk->mik', gram, gram, precision=lax.Precision.HIGHEST)
            iterate = 3.4445 * iterate + jnp.einsum('mij,mjk->mik', mixed, iterate, precision=lax.Precision.HIGHEST)
        return iterate[0]
    iterate = lax.map(orthogonal_one, new_momentum)
    new_weights = weight_stack - learn_rate * iterate
    return (new_weights, new_momentum)
```

```python
import functools

import jax
import jax.numpy as jnp
from jax import lax
from jax.experimental import pallas as pl
from jax.experimental.pallas import tpu as pltpu
from jax.sharding import PartitionSpec as P

ITERS = 5
RING = 4
CHUNKS = 4
AHEAD = 2

hold_rate = 0.95
learn_rate = 1.0

MESH = pl.DeviceIdType.MESH


def mul(a, b):
    return lax.dot_general(
        a, b, (((1,), (0,)), ((), ())),
        precision=lax.Precision.HIGHEST, preferred_element_type=jnp.float32,
    )


def mul_t(a, b):
    return lax.dot_general(
        a, b, (((1,), (1,)), ((), ())),
        precision=lax.Precision.HIGHEST, preferred_element_type=jnp.float32,
    )


def spread(packed, side):
    first = lax.broadcasted_iota(jnp.int32, (side, 2 * side), 1) < side
    return jnp.concatenate(
        [jnp.where(first, packed, 0.0), jnp.where(first, 0.0, packed)], axis=0
    )


def transform(packed, side):
    wide = 2 * side
    row = lax.broadcasted_iota(jnp.int32, (side, wide), 0)
    lane = lax.broadcasted_iota(jnp.int32, (side, wide), 1)
    first = lane < side
    scales = [
        lax.rsqrt(
            jnp.sum(
                jnp.sum(jnp.where(lane == row + at, packed, 0.0), axis=1, keepdims=True),
                axis=0, keepdims=True,
            ) + 1e-06
        )
        for at in (0, side)
    ]
    scale = jnp.where(first, scales[0], scales[1])
    gram = spread(packed * scale * scale, side)
    eye = lax.broadcasted_iota(jnp.int32, (wide, wide), 0) == lax.broadcasted_iota(
        jnp.int32, (wide, wide), 1
    )
    total = None
    for step in range(ITERS):
        factor = jnp.where(eye, 3.4445, 0.0) + (-4.775 * gram + 2.0315 * mul(gram, gram))
        total = factor if total is None else mul(factor, total)
        if step < ITERS - 1:
            gram = mul(factor, mul(factor, gram))
    return jnp.where(first, total[:side], total[side:]) * scale


def kernel(
    cols, mom, back, mid, held, made, omid, xs, obuf, mine, theirs, fac,
    in1_s, in1_r, in2_s, in2_r, in3_s, in3_r, rs_s, rs_r, ag_s, ag_r,
    o1_s, o1_r, o2_s, o2_r, o3_s, o3_r, own_sem,
):
    me, col = lax.axis_index("rows"), lax.axis_index("cols")
    z, y = me // RING, lax.rem(me, RING)
    place, core = col // 2, lax.rem(col, 2)
    mats, share, width = mom.shape[2:]
    side = RING * RING * share
    count = mats // CHUNKS
    half = count // 2
    pairs = count // 2
    others = range(1, RING)
    order = (1, 3, 2)

    def up(at, k):
        return lax.rem(at + k, RING)

    def down(at, k):
        return lax.rem(at + RING - k, RING)

    def along(h, at):
        return (z * RING + at, col) if h == 0 else (at * RING + y, col)

    def col_peer(k):
        return lax.rem(col + k, cols)

    barrier = pltpu.get_barrier_semaphore()
    for k in others:
        for h in (0, 1):
            pl.semaphore_signal(
                barrier, inc=1, device_id=along(h, up((y, z)[h], k)), device_id_type=MESH
            )
    for k in range(1, cols):
        pl.semaphore_signal(barrier, inc=1, device_id=(me, col_peer(k)), device_id_type=MESH)
    pl.semaphore_wait(barrier, 2 * (RING - 1) + cols - 1)

    def remote(src, dst, send, recv, to):
        return pltpu.make_async_remote_copy(
            src_ref=src, dst_ref=dst, send_sem=send, recv_sem=recv,
            device_id=to, device_id_type=MESH,
        )

    def of(h, c):
        return pl.ds(c * count + h * half, half), pl.ds(c * half, half)

    def in1(c, h, k):
        at, near = of(h, c)
        to = up((y, z)[h], k)
        src = mom.at[:, to, at] if h == 0 else mom.at[to, :, at]
        return remote(src, mid.at[h, k, :, near], in1_s.at[c, h, k], in1_r.at[c, h, k], along(h, to))

    def in2(c, h, k):
        at, near = of(h, c)
        to = up((z, y)[h], k)
        dst = held.at[k, pl.ds(1, RING - 1), at] if h == 0 else held.at[pl.ds(1, RING - 1), k, at]
        return remote(
            mid.at[h, pl.ds(1, RING - 1), to, near], dst,
            in2_s.at[c, h, k], in2_r.at[c, h, k], along(1 - h, to),
        )

    def in3(c, h, k):
        at, _ = of(h, c)
        to = up((z, y)[h], k)
        src, dst = (
            (mom.at[to, y, at], held.at[k, 0, at]) if h == 0
            else (mom.at[z, to, at], held.at[0, k, at])
        )
        return remote(src, dst, in3_s.at[c, h, k], in3_r.at[c, h, k], along(1 - h, to))

    def out1(c, h, k):
        at, near = of(h, c)
        to = down((z, y)[h], k)
        src, dst = (
            (made.at[k, pl.ds(1, RING - 1), at], omid.at[0, pl.ds(1, RING - 1), z, near]) if h == 0
            else (made.at[pl.ds(1, RING - 1), k, at], omid.at[1, pl.ds(1, RING - 1), y, near])
        )
        return remote(src, dst, o1_s.at[c, h, k], o1_r.at[c, h, k], along(1 - h, to))

    def out3(c, h, k):
        at, _ = of(h, c)
        to = down((z, y)[h], k)
        src = made.at[k, 0, at] if h == 0 else made.at[0, k, at]
        return remote(
            src, back.at[z, y, at], o3_s.at[c, h, k], o3_r.at[c, h, k], along(1 - h, to)
        )

    def out2(c, h, k):
        at, near = of(h, c)
        to = down((y, z)[h], k)
        dst = back.at[:, y, at] if h == 0 else back.at[z, :, at]
        return remote(
            omid.at[h, k, :, near], dst, o2_s.at[c, h, k], o2_r.at[c, h, k], along(h, to)
        )

    def own_back(c):
        at = pl.ds(c * count, count)
        return pltpu.make_async_copy(made.at[0, 0, at], back.at[z, y, at], own_sem.at[c + 1])

    def worker(c, p):
        return 2 * p + lax.rem(c, 2)

    def gram_send(c, p):
        to = worker(c, p)
        k = lax.rem(col + cols - to, cols)
        return remote(
            mine.at[c, p], theirs.at[c, k], rs_s.at[c, p], rs_r.at[c, k], (me, to)
        )

    def gram_recv(c, k):
        return remote(
            mine.at[c, 0], theirs.at[c, k], rs_s.at[c, 0], rs_r.at[c, k], (me, col_peer(k))
        )

    def fac_copy(c, p, k):
        return remote(
            fac.at[c, p], fac.at[c, p], ag_s.at[c, k], ag_r.at[c, p], (me, col_peer(k))
        )

    own_in = pltpu.make_async_copy(mom.at[z, y], held.at[0, 0], own_sem.at[0])
    own_in.start()

    def start_in1(c):
        for k in order:
            for h in (0, 1):
                in1(c, h, k).start()

    for c in range(AHEAD):
        start_in1(c)
    own_in.wait()

    def rows_of(h, i, m, near):
        dz, dy = i // RING, i % RING
        if h == 0 and dz == 0 and dy > 0:
            return mid[0, dy, z, near]
        if h == 1 and dy == 0 and dz > 0:
            return mid[1, dz, y, near]
        return held[dz, dy, m]

    def keep_rows(h, i, m, near, value):
        dz, dy = i // RING, i % RING
        if h == 0 and dz == 0 and dy > 0:
            omid[0, dy, z, near] = value
        elif h == 1 and dy == 0 and dz > 0:
            omid[1, dz, y, near] = value
        else:
            made[dz, dy, m] = value

    def gram_stage(c):
        for k in others:
            for h in (0, 1):
                in2(c, h, k).wait_recv()
                in3(c, h, k).wait_recv()
        first = lax.broadcasted_iota(jnp.int32, (side, 2 * side), 1) < side

        @pl.loop(0, pairs // 2)
        def _(q):
            for h in (0, 1):
                p = h * (pairs // 2) + q
                for at in (0, 1):
                    near = c * half + 2 * q + at
                    m = c * count + h * half + 2 * q + at
                    for i in range(RING * RING):
                        xs[c, p, pl.ds(at * side + i * share, share), :] = rows_of(h, i, m, near)
            for h in (0, 1):
                p = h * (pairs // 2) + q
                x = xs[c, p]
                both = mul_t(x, x)
                mine[c, p] = jnp.where(first, both[:side], both[side:])

        for p in range(pairs):
            @pl.when(worker(c, p) != col)
            def _():
                gram_send(c, p).start()

    def transform_stage(c):
        @pl.when(core == lax.rem(c, 2))
        def _():
            for k in range(1, cols):
                gram_recv(c, k).wait_recv()
            one = mine[c, place]
            for k in range(1, cols):
                one = one + theirs[c, k]
            fac[c, place] = transform(one, side)
            for k in range(1, cols):
                fac_copy(c, place, k).start()

    def apply_stage(c):
        for p in range(pairs):
            @pl.when(worker(c, p) != col)
            def _():
                fac_copy(c, p, 1).wait_recv()

        @pl.loop(0, pairs // 2)
        def _(q):
            for h in (0, 1):
                p = h * (pairs // 2) + q
                obuf[h] = mul(spread(fac[c, p], side), xs[c, p])
            for h in (0, 1):
                for at in (0, 1):
                    near = c * half + 2 * q + at
                    m = c * count + h * half + 2 * q + at
                    for i in range(RING * RING):
                        keep_rows(h, i, m, near, obuf[h, pl.ds(at * side + i * share, share), :])

        for k in order:
            for h in (0, 1):
                out1(c, h, k).start()
                out3(c, h, k).start()
        own_back(c).start()

    @pl.loop(0, CHUNKS + 4)
    def _(t):
        @pl.when(t < CHUNKS)
        def _():
            for k in order:
                for h in (0, 1):
                    in1(t, h, k).wait_recv()
            for k in order:
                for h in (0, 1):
                    in2(t, h, k).start()
                    in3(t, h, k).start()

        @pl.when(t + AHEAD < CHUNKS)
        def _():
            start_in1(t + AHEAD)

        @pl.when(t >= 4)
        def _():
            c = t - 4
            for k in order:
                for h in (0, 1):
                    out1(c, h, k).wait_recv()
            for k in order:
                for h in (0, 1):
                    out2(c, h, k).start()

        @pl.when((t >= 1) & (t < CHUNKS + 1))
        def _():
            gram_stage(t - 1)

        @pl.when((t >= 2) & (t < CHUNKS + 2))
        def _():
            transform_stage(t - 2)

        @pl.when((t >= 3) & (t < CHUNKS + 3))
        def _():
            apply_stage(t - 3)

    @pl.loop(0, CHUNKS)
    def _(c):
        for k in others:
            for h in (0, 1):
                in1(c, h, k).wait_send()
                in2(c, h, k).wait_send()
                in3(c, h, k).wait_send()
                out1(c, h, k).wait_send()
                out2(c, h, k).wait()
                out3(c, h, k).wait()
        for p in range(pairs):
            @pl.when(worker(c, p) != col)
            def _():
                gram_send(c, p).wait_send()

        @pl.when(core == lax.rem(c, 2))
        def _():
            for k in range(1, cols):
                fac_copy(c, place, k).wait_send()
        own_back(c).wait()


def exchange_and_iterate(new_momentum, cols):
    every, share, width = new_momentum.shape
    mats = every // (RING * RING)
    side = RING * RING * share
    count = mats // CHUNKS
    pairs = count // 2
    f32, dma = jnp.float32, pltpu.SemaphoreType.DMA
    hops = dma((CHUNKS, 2, RING))
    shape = (RING, RING, mats, share, width)
    out = pl.pallas_call(
        functools.partial(kernel, cols),
        out_shape=jax.ShapeDtypeStruct(shape, f32),
        in_specs=[pl.BlockSpec(memory_space=pl.ANY)],
        out_specs=pl.BlockSpec(memory_space=pl.ANY),
        scratch_shapes=[
            pltpu.VMEM((2, RING, RING, mats // 2, share, width), f32),
            pltpu.VMEM(shape, f32),
            pltpu.VMEM(shape, f32),
            pltpu.VMEM((2, RING, RING, mats // 2, share, width), f32),
            pltpu.VMEM((CHUNKS, pairs, 2 * side, width), f32),
            pltpu.VMEM((2, 2 * side, width), f32),
            pltpu.VMEM((CHUNKS, pairs, side, 2 * side), f32),
            pltpu.VMEM((CHUNKS, cols, side, 2 * side), f32),
            pltpu.VMEM((CHUNKS, pairs, side, 2 * side), f32),
            hops, hops, hops, hops, hops, hops,
            dma((CHUNKS, pairs)), dma((CHUNKS, cols)),
            dma((CHUNKS, cols)), dma((CHUNKS, pairs)),
            hops, hops, hops, hops, hops, hops,
            dma((CHUNKS + 1,)),
        ],
        compiler_params=pltpu.CompilerParams(
            collective_id=0, has_side_effects=True, vmem_limit_bytes=40 * 2**20
        ),
        name="exchange_and_iterate",
    )(new_momentum.reshape(shape))
    return out.reshape(every, share, width)


def solution(mesh):
    cols = mesh.shape["cols"]

    def on_device(grad_stack, moment_stack, weight_stack):
        new_momentum = hold_rate * moment_stack + grad_stack
        back = exchange_and_iterate(new_momentum, cols)
        new_weights = weight_stack - learn_rate * back
        return (new_weights, new_momentum)

    placed = P(None, "rows", "cols")
    return jax.shard_map(
        on_device,
        mesh=mesh,
        in_specs=(placed, placed, placed),
        out_specs=(placed, placed),
        check_vma=False,
    )
```

```python
import functools

import jax
import jax.numpy as jnp
from jax import lax
from jax.experimental import pallas as pl
from jax.experimental.pallas import tpu as pltpu
from jax.sharding import PartitionSpec as P

ITERS = 5
RING = 4
CHUNKS = 8
OUT_HOPS = 2
SCHEDULE = (
    "M0", "M4", "B0", "S4", "M2", "M1", "M5", "M3", "S3", "S1", "S2", "I4", "I3", "I1",
    "I2", "S5", "S0", "G4", "G3", "M6", "M7", "S6", "S7", "G1", "G2", "I5", "T4", "I0",
    "T3", "I6", "T1", "I7", "T2", "A4", "G5", "A3", "G0", "G6", "A1", "G7", "A2", "O4",
    "T5", "O3", "T6", "T0", "O1", "T7", "O2", "A5", "A0", "A6", "A7", "O5", "O0", "O6",
    "O7",
)

hold_rate = 0.95
learn_rate = 1.0

MESH = pl.DeviceIdType.MESH


def mul(a, b):
    return lax.dot_general(
        a, b, (((1,), (0,)), ((), ())),
        precision=lax.Precision.HIGHEST, preferred_element_type=jnp.float32,
    )


def mul_t(a, b):
    return lax.dot_general(
        a, b, (((1,), (1,)), ((), ())),
        precision=lax.Precision.HIGHEST, preferred_element_type=jnp.float32,
    )


def spread(packed, side):
    first = lax.broadcasted_iota(jnp.int32, (side, 2 * side), 1) < side
    return jnp.concatenate(
        [jnp.where(first, packed, 0.0), jnp.where(first, 0.0, packed)], axis=0
    )


def parts(x):
    high = x.astype(jnp.bfloat16)
    rest = x - high.astype(jnp.float32)
    mid = rest.astype(jnp.bfloat16)
    low = (rest - mid.astype(jnp.float32)).astype(jnp.bfloat16)
    return high, mid, low


def right(x, side):
    high, mid, low = (part.astype(jnp.bfloat16) for part in map(
        lambda part: spread(part.astype(jnp.float32), side), parts(x)
    ))
    both = jnp.concatenate(
        [jnp.concatenate([high, mid], axis=1), jnp.concatenate([mid, high], axis=1)], axis=0
    )
    return both, jnp.concatenate([low, high], axis=0)


def times(x, factors):
    both, rest = factors
    wide = rest.shape[1]
    high, mid, low = parts(x)

    def dot(a, b):
        return jnp.dot(a, b, preferred_element_type=jnp.float32)

    large = dot(jnp.concatenate([high, mid], axis=1), both)
    small = dot(jnp.concatenate([high, low], axis=1), rest)
    return large[:, :wide] + (large[:, wide:] + small)


def transform(packed, side):
    wide = 2 * side
    row = lax.broadcasted_iota(jnp.int32, (side, wide), 0)
    lane = lax.broadcasted_iota(jnp.int32, (side, wide), 1)
    first = lane < side
    scales = [
        lax.rsqrt(
            jnp.sum(
                jnp.sum(jnp.where(lane == row + at, packed, 0.0), axis=1, keepdims=True),
                axis=0, keepdims=True,
            ) + 1e-06
        )
        for at in (0, side)
    ]
    scale = jnp.where(first, scales[0], scales[1])
    gram = packed * scale * scale
    eye = jnp.where((lane == row) | (lane == row + side), 3.4445, 0.0)
    total = None
    for step in range(ITERS):
        factor = eye + (-4.775 * gram + 2.0315 * times(gram, right(gram, side)))
        factors = right(factor, side)
        if step == ITERS - 1:
            total = times(total, factors)
        elif total is None:
            total = factor
            gram = times(times(gram, factors), factors)
        else:
            pair = times(jnp.concatenate([gram, total], axis=0), factors)
            gram, total = times(pair[:side], factors), pair[side:]
    return total * scale


def kernel(
    cols, grad, moment, back, mom, old, mid, held, made, omid, xs, obuf, mine, theirs, fac,
    load_sem, in1_r, in2_r, o1_r, end_r, rs_r, ag_r, sent,
):
    me, col = lax.axis_index("rows"), lax.axis_index("cols")
    z, y = me // RING, lax.rem(me, RING)
    mats, share, width = mom.shape[2:]
    side = RING * RING * share
    count = mats // CHUNKS
    half = count // 2
    pairs = count // 2
    workers = cols // pairs
    others = range(1, RING)
    order = (1, 3, 2)
    after = pl.ds(1, RING - 1)

    def up(at, k):
        return lax.rem(at + k, RING)

    def down(at, k):
        return lax.rem(at + RING - k, RING)

    def along(h, at):
        return (z * RING + at, col) if h == 0 else (at * RING + y, col)

    def col_peer(k):
        return lax.rem(col + k, cols)

    def all_of(ref, sem):
        pltpu.make_async_copy(ref, ref, sem).wait()

    def remote(src, dst, send, recv, to):
        return pltpu.make_async_remote_copy(
            src_ref=src, dst_ref=dst, send_sem=send, recv_sem=recv,
            device_id=to, device_id_type=MESH,
        )

    barrier = pltpu.get_barrier_semaphore()
    for k in others:
        for h in (0, 1):
            pl.semaphore_signal(
                barrier, inc=1, device_id=along(h, up((y, z)[h], k)), device_id_type=MESH
            )
    for k in range(1, cols):
        pl.semaphore_signal(barrier, inc=1, device_id=(me, col_peer(k)), device_id_type=MESH)

    def load(c):
        at = pl.ds(c * count, count)
        return [
            pltpu.make_async_copy(src.at[:, :, at], dst.at[:, :, at], load_sem.at[n, c])
            for n, (src, dst) in enumerate(((grad, mom), (moment, old)))
        ]

    for c in range(CHUNKS):
        for copy in load(c):
            copy.start()

    def meet(_):
        pl.semaphore_wait(barrier, 2 * (RING - 1) + cols - 1)

    def momentum_stage(c):
        for copy in load(c):
            copy.wait()

        @pl.loop(0, RING * RING)
        def _(i):
            at = (i // RING, lax.rem(i, RING), pl.ds(c * count, count))
            mom[at] = hold_rate * old[at] + mom[at]

    def of(h, c):
        return pl.ds(c * count + h * half, half), pl.ds(c * half, half)

    def in1(c, h, k):
        at, near = of(h, c)
        to = up((y, z)[h], k)
        src = mom.at[:, to, at] if h == 0 else mom.at[to, :, at]
        return remote(src, mid.at[h, k, :, near], sent.at[0], in1_r.at[c], along(h, to))

    def in2(c, h, k):
        at, near = of(h, c)
        to = up((z, y)[h], k)
        dst = held.at[k, after, at] if h == 0 else held.at[after, k, at]
        return remote(mid.at[h, after, to, near], dst, sent.at[1], in2_r.at[c], along(1 - h, to))

    def in3(c, h, k):
        at, _ = of(h, c)
        to = up((z, y)[h], k)
        src, dst = (
            (mom.at[to, y, at], held.at[k, 0, at]) if h == 0
            else (mom.at[z, to, at], held.at[0, k, at])
        )
        return remote(src, dst, sent.at[2], in2_r.at[c], along(1 - h, to))

    def out1(c, h, k):
        at, near = of(h, c)
        to = down((z, y)[h], k)
        src, dst = (
            (made.at[k, after, at], omid.at[0, after, z, near]) if h == 0
            else (made.at[after, k, at], omid.at[1, after, y, near])
        )
        return remote(src, dst, sent.at[3], o1_r.at[c], along(1 - h, to))

    def out3(c, h, k):
        at, _ = of(h, c)
        to = down((z, y)[h], k)
        src = made.at[k, 0, at] if h == 0 else made.at[0, k, at]
        return remote(src, back.at[z, y, at], sent.at[4], end_r.at[0], along(1 - h, to))

    def out2(c, h, k):
        at, near = of(h, c)
        to = down((y, z)[h], k)
        dst = back.at[:, y, at] if h == 0 else back.at[z, :, at]
        return remote(omid.at[h, k, :, near], dst, sent.at[5], end_r.at[1], along(h, to))

    def out(c, dz, dy):
        at = pl.ds(c * count, count)
        n = 0 if dz == 0 else 1
        return remote(
            made.at[dz, dy, at], back.at[z, y, at], sent.at[3 + n], end_r.at[n],
            (down(z, dz) * RING + down(y, dy), col),
        )

    def worker(c, p):
        return workers * p + c % workers

    def gram_send(c, p):
        to = worker(c, p)
        k = lax.rem(col + cols - to, cols)
        return remote(mine.at[c, p], theirs.at[c, k], sent.at[6], rs_r.at[c], (me, to))

    def fac_send(c, p, k):
        return remote(fac.at[c, p], fac.at[c, p], sent.at[7], ag_r.at[c], (me, col_peer(k)))

    def start_in1(c):
        for k in order:
            for h in (0, 1):
                in1(c, h, k).start()

    def rows_of(h, i, m, near):
        dz, dy = i // RING, i % RING
        if i == 0:
            return mom[z, y, m]
        if h == 0 and dz == 0:
            return mid[0, dy, z, near]
        if h == 1 and dy == 0:
            return mid[1, dz, y, near]
        return held[dz, dy, m]

    def keep_rows(h, i, m, near, value):
        dz, dy = i // RING, i % RING
        if i == 0:
            back[z, y, m] = value
        elif OUT_HOPS == 2 and h == 0 and dz == 0:
            omid[0, dy, z, near] = value
        elif OUT_HOPS == 2 and h == 1 and dy == 0:
            omid[1, dz, y, near] = value
        else:
            made[dz, dy, m] = value

    def gram_stage(c):
        all_of(held.at[after, :, pl.ds(c * count, count)], in2_r.at[c])
        first = lax.broadcasted_iota(jnp.int32, (side, 2 * side), 1) < side

        @pl.loop(0, pairs // 2)
        def _(q):
            for h in (0, 1):
                p = h * (pairs // 2) + q
                for at in (0, 1):
                    near = c * half + 2 * q + at
                    m = c * count + h * half + 2 * q + at
                    for i in range(RING * RING):
                        xs[c, p, pl.ds(at * side + i * share, share), :] = rows_of(h, i, m, near)
            for h in (0, 1):
                p = h * (pairs // 2) + q
                x = xs[c, p]
                both = mul_t(x, x)
                mine[c, p] = jnp.where(first, both[:side], both[side:])

        for p in range(pairs):
            @pl.when(worker(c, p) != col)
            def _():
                gram_send(c, p).start()

    def works(c):
        return lax.rem(col, workers) == c % workers

    def transform_stage(c):
        @pl.when(works(c))
        def _():
            place = col // workers
            all_of(theirs.at[c, pl.ds(1, cols - 1)], rs_r.at[c])
            one = mine[c, place]
            for k in range(1, cols):
                one = one + theirs[c, k]
            fac[c, place] = transform(one, side)
            for k in range(1, cols):
                fac_send(c, place, k).start()

    def apply_stage(c):
        @pl.when(works(c))
        def _():
            all_of(fac.at[c, pl.ds(0, pairs - 1)], ag_r.at[c])

        @pl.when(jnp.logical_not(works(c)))
        def _():
            all_of(fac.at[c], ag_r.at[c])

        @pl.loop(0, pairs // 2)
        def _(q):
            for h in (0, 1):
                p = h * (pairs // 2) + q
                obuf[h] = mul(spread(fac[c, p], side), xs[c, p])
            for h in (0, 1):
                for at in (0, 1):
                    near = c * half + 2 * q + at
                    m = c * count + h * half + 2 * q + at
                    for i in range(RING * RING):
                        keep_rows(h, i, m, near, obuf[h, pl.ds(at * side + i * share, share), :])

        if OUT_HOPS == 2:
            for k in order:
                for h in (0, 1):
                    out1(c, h, k).start()
                    out3(c, h, k).start()
        else:
            for dz, dy in FAR:
                out(c, dz, dy).start()

    def forward_in(c):
        all_of(mid.at[:, after, :, pl.ds(c * half, half)], in1_r.at[c])
        for k in order:
            for h in (0, 1):
                in2(c, h, k).start()
                in3(c, h, k).start()

    def forward_out(c):
        if OUT_HOPS == 2:
            all_of(omid.at[:, after, after, pl.ds(c * half, half)], o1_r.at[c])
            for k in order:
                for h in (0, 1):
                    out2(c, h, k).start()

    stages = {
        "M": momentum_stage, "B": meet, "S": start_in1, "I": forward_in, "G": gram_stage,
        "T": transform_stage, "A": apply_stage, "O": forward_out,
    }
    for event in SCHEDULE:
        stages[event[0]](int(event[1:]))

    if OUT_HOPS == 2:
        all_of(back.at[0, after], end_r.at[0])
        all_of(back.at[after], end_r.at[1])
        all_of(made.at[after, after], sent.at[3])
        all_of(made.at[0, after], sent.at[4])
        all_of(made.at[after], sent.at[5])
    else:
        all_of(back.at[0, after], end_r.at[0])
        all_of(back.at[after], end_r.at[1])
        all_of(made.at[0, after], sent.at[3])
        all_of(made.at[after], sent.at[4])
    all_of(mom.at[after], sent.at[0])
    all_of(mom.at[after, after], sent.at[1])
    all_of(mom.at[0, after], sent.at[2])
    all_of(theirs.at[pl.ds(0, 2), pl.ds(1, cols - 1)], sent.at[6])
    all_of(theirs.at[pl.ds(0, 2), pl.ds(1, cols - 1)], sent.at[7])


FAR = [(2, 2), (2, 3), (3, 2), (2, 1), (1, 2), (2, 0), (0, 2), (3, 1), (1, 3), (3, 3), (1, 1), (3, 0), (0, 3), (1, 0), (0, 1)]


def exchange_and_iterate(grad, moment, cols):
    every, share, width = grad.shape
    mats = every // (RING * RING)
    side = RING * RING * share
    count = mats // CHUNKS
    pairs = count // 2
    f32, dma = jnp.float32, pltpu.SemaphoreType.DMA
    shape = (RING, RING, mats, share, width)
    halves = (2, RING, RING, mats // 2, share, width)
    whole = pl.BlockSpec(memory_space=pltpu.VMEM)
    back, mom = pl.pallas_call(
        functools.partial(kernel, cols),
        out_shape=[jax.ShapeDtypeStruct(shape, f32)] * 2,
        in_specs=[pl.BlockSpec(memory_space=pltpu.HBM)] * 2,
        out_specs=[whole, whole],
        scratch_shapes=[
            pltpu.VMEM(shape, f32),
            pltpu.VMEM(halves, f32),
            pltpu.VMEM(shape, f32),
            pltpu.VMEM(shape, f32),
            pltpu.VMEM(halves, f32),
            pltpu.VMEM((CHUNKS, pairs, 2 * side, width), f32),
            pltpu.VMEM((2, 2 * side, width), f32),
            pltpu.VMEM((CHUNKS, pairs, side, 2 * side), f32),
            pltpu.VMEM((CHUNKS, cols, side, 2 * side), f32),
            pltpu.VMEM((CHUNKS, pairs, side, 2 * side), f32),
            dma((2, CHUNKS)), dma((CHUNKS,)), dma((CHUNKS,)), dma((CHUNKS,)), dma((2,)),
            dma((CHUNKS,)), dma((CHUNKS,)), dma((8,)),
        ],
        compiler_params=pltpu.CompilerParams(
            collective_id=0, has_side_effects=True, vmem_limit_bytes=40 * 2**20
        ),
        name="exchange_and_iterate",
    )(*(pltpu.with_memory_space_constraint(v.reshape(shape), pltpu.HBM) for v in (grad, moment)))
    return back.reshape(grad.shape), mom.reshape(grad.shape)


def solution(mesh):
    cols = mesh.shape["cols"]

    def on_device(grad_stack, moment_stack, weight_stack):
        back, new_momentum = exchange_and_iterate(grad_stack, moment_stack, cols)
        new_weights = weight_stack - learn_rate * back
        return (new_weights, new_momentum)

    placed = P(None, "rows", "cols")
    return jax.shard_map(
        on_device,
        mesh=mesh,
        in_specs=(placed, placed, placed),
        out_specs=(placed, placed),
        check_vma=False,
    )
```

```python
import functools

import jax
import jax.numpy as jnp
from jax import lax
from jax.experimental import pallas as pl
from jax.experimental.pallas import tpu as pltpu
from jax.sharding import PartitionSpec as P

ITERS = 5
RING = 4
CHUNKS = 8
OUT_HOPS = 2
SCHEDULE = (
    "M1", "B0", "S1", "M5", "M0", "M7", "M4", "S0", "S7", "S5", "I1", "M6", "I0", "I7",
    "I5", "G1", "M2", "S2", "G0", "S4", "M3", "S6", "S3", "G7", "G5", "I2", "T1", "T0",
    "I4", "T7", "I6", "T5", "I3", "A1", "G2", "A0", "G4", "A7", "G6", "G3", "A5", "O1",
    "T2", "O0", "T4", "O7", "T3", "T6", "O5", "A2", "A4", "A6", "A3", "O2", "O4", "O6",
    "O3",
)

hold_rate = 0.95
learn_rate = 1.0

MESH = pl.DeviceIdType.MESH


def mul(a, b):
    return lax.dot_general(
        a, b, (((1,), (0,)), ((), ())),
        precision=lax.Precision.HIGHEST, preferred_element_type=jnp.float32,
    )


def mul_t(a, b):
    return lax.dot_general(
        a, b, (((1,), (1,)), ((), ())),
        precision=lax.Precision.HIGHEST, preferred_element_type=jnp.float32,
    )


def spread(packed, side):
    first = lax.broadcasted_iota(jnp.int32, (side, 2 * side), 1) < side
    return jnp.concatenate(
        [jnp.where(first, packed, 0.0), jnp.where(first, 0.0, packed)], axis=0
    )


def parts(x):
    high = x.astype(jnp.bfloat16)
    rest = x - high.astype(jnp.float32)
    mid = rest.astype(jnp.bfloat16)
    low = (rest - mid.astype(jnp.float32)).astype(jnp.bfloat16)
    return high, mid, low


def right(x, side):
    high, mid, low = (part.astype(jnp.bfloat16) for part in map(
        lambda part: spread(part.astype(jnp.float32), side), parts(x)
    ))
    both = jnp.concatenate(
        [jnp.concatenate([high, mid], axis=1), jnp.concatenate([mid, high], axis=1)], axis=0
    )
    return both, jnp.concatenate([low, high], axis=0)


def times(x, factors):
    both, rest = factors
    wide = rest.shape[1]
    high, mid, low = parts(x)

    def dot(a, b):
        return jnp.dot(a, b, preferred_element_type=jnp.float32)

    large = dot(jnp.concatenate([high, mid], axis=1), both)
    small = dot(jnp.concatenate([high, low], axis=1), rest)
    return large[:, :wide] + (large[:, wide:] + small)


def transform(packed, side):
    wide = 2 * side
    row = lax.broadcasted_iota(jnp.int32, (side, wide), 0)
    lane = lax.broadcasted_iota(jnp.int32, (side, wide), 1)
    first = lane < side
    scales = [
        lax.rsqrt(
            jnp.sum(
                jnp.sum(jnp.where(lane == row + at, packed, 0.0), axis=1, keepdims=True),
                axis=0, keepdims=True,
            ) + 1e-06
        )
        for at in (0, side)
    ]
    scale = jnp.where(first, scales[0], scales[1])
    gram = packed * scale * scale
    eye = jnp.where((lane == row) | (lane == row + side), 3.4445, 0.0)
    total = None
    for step in range(ITERS):
        factor = eye + (-4.775 * gram + 2.0315 * times(gram, right(gram, side)))
        factors = right(factor, side)
        if step == ITERS - 1:
            total = times(total, factors)
        elif total is None:
            total = factor
            gram = times(times(gram, factors), factors)
        else:
            pair = times(jnp.concatenate([gram, total], axis=0), factors)
            gram, total = times(pair[:side], factors), pair[side:]
    return total * scale


def kernel(
    cols, grad, moment, back, mom, old, mid, held, made, omid, xs, obuf, mine, theirs, fac,
    load_sem, in1_r, in2_r, o1_r, end_r, rs_r, ag_r, sent,
):
    me, col = lax.axis_index("rows"), lax.axis_index("cols")
    z, y = me // RING, lax.rem(me, RING)
    mats, share, width = mom.shape[2:]
    side = RING * RING * share
    count = mats // CHUNKS
    half = count // 2
    pairs = count // 2
    workers = cols // pairs
    others = range(1, RING)
    order = (1, 3, 2)
    after = pl.ds(1, RING - 1)

    def up(at, k):
        return lax.rem(at + k, RING)

    def down(at, k):
        return lax.rem(at + RING - k, RING)

    def along(h, at):
        return (z * RING + at, col) if h == 0 else (at * RING + y, col)

    def col_peer(k):
        return lax.rem(col + k, cols)

    def all_of(ref, sem):
        pltpu.make_async_copy(ref, ref, sem).wait()

    def remote(src, dst, send, recv, to):
        return pltpu.make_async_remote_copy(
            src_ref=src, dst_ref=dst, send_sem=send, recv_sem=recv,
            device_id=to, device_id_type=MESH,
        )

    barrier = pltpu.get_barrier_semaphore()
    for k in others:
        for h in (0, 1):
            pl.semaphore_signal(
                barrier, inc=1, device_id=along(h, up((y, z)[h], k)), device_id_type=MESH
            )
    for k in range(1, cols):
        pl.semaphore_signal(barrier, inc=1, device_id=(me, col_peer(k)), device_id_type=MESH)

    def load(c):
        at = pl.ds(c * count, count)
        return [
            pltpu.make_async_copy(src.at[:, :, at], dst.at[:, :, at], load_sem.at[n, c])
            for n, (src, dst) in enumerate(((grad, mom), (moment, old)))
        ]

    for c in range(CHUNKS):
        for copy in load(c):
            copy.start()

    def meet(_):
        pl.semaphore_wait(barrier, 2 * (RING - 1) + cols - 1)

    def momentum_stage(c):
        for copy in load(c):
            copy.wait()

        @pl.loop(0, RING * RING)
        def _(i):
            at = (i // RING, lax.rem(i, RING), pl.ds(c * count, count))
            mom[at] = hold_rate * old[at] + mom[at]

    def of(h, c):
        return pl.ds(c * count + h * half, half), pl.ds(c * half, half)

    def in1(c, h, k):
        at, near = of(h, c)
        to = up((y, z)[h], k)
        src = mom.at[:, to, at] if h == 0 else mom.at[to, :, at]
        return remote(src, mid.at[h, k, :, near], sent.at[0], in1_r.at[c], along(h, to))

    def in2(c, h, k):
        at, near = of(h, c)
        to = up((z, y)[h], k)
        dst = held.at[k, after, at] if h == 0 else held.at[after, k, at]
        return remote(mid.at[h, after, to, near], dst, sent.at[1], in2_r.at[c], along(1 - h, to))

    def in3(c, h, k):
        at, _ = of(h, c)
        to = up((z, y)[h], k)
        src, dst = (
            (mom.at[to, y, at], held.at[k, 0, at]) if h == 0
            else (mom.at[z, to, at], held.at[0, k, at])
        )
        return remote(src, dst, sent.at[2], in2_r.at[c], along(1 - h, to))

    def out1(c, h, k):
        at, near = of(h, c)
        to = down((z, y)[h], k)
        src, dst = (
            (made.at[k, after, at], omid.at[0, after, z, near]) if h == 0
            else (made.at[after, k, at], omid.at[1, after, y, near])
        )
        return remote(src, dst, sent.at[3], o1_r.at[c], along(1 - h, to))

    def out3(c, h, k):
        at, _ = of(h, c)
        to = down((z, y)[h], k)
        src = made.at[k, 0, at] if h == 0 else made.at[0, k, at]
        return remote(src, back.at[z, y, at], sent.at[4], end_r.at[0], along(1 - h, to))

    def out2(c, h, k):
        at, near = of(h, c)
        to = down((y, z)[h], k)
        dst = back.at[:, y, at] if h == 0 else back.at[z, :, at]
        return remote(omid.at[h, k, :, near], dst, sent.at[5], end_r.at[1], along(h, to))

    def out(c, dz, dy):
        at = pl.ds(c * count, count)
        n = 0 if dz == 0 else 1
        return remote(
            made.at[dz, dy, at], back.at[z, y, at], sent.at[3 + n], end_r.at[n],
            (down(z, dz) * RING + down(y, dy), col),
        )

    def worker(c, p):
        return workers * p + c % workers

    def gram_send(c, p):
        to = worker(c, p)
        k = lax.rem(col + cols - to, cols)
        return remote(mine.at[c, p], theirs.at[c, k], sent.at[6], rs_r.at[c], (me, to))

    def fac_send(c, p, k):
        return remote(fac.at[c, p], fac.at[c, p], sent.at[7], ag_r.at[c], (me, col_peer(k)))

    def start_in1(c):
        for k in order:
            for h in (0, 1):
                in1(c, h, k).start()

    def rows_of(h, i, m, near):
        dz, dy = i // RING, i % RING
        if i == 0:
            return mom[z, y, m]
        if h == 0 and dz == 0:
            return mid[0, dy, z, near]
        if h == 1 and dy == 0:
            return mid[1, dz, y, near]
        return held[dz, dy, m]

    def keep_rows(h, i, m, near, value):
        dz, dy = i // RING, i % RING
        if i == 0:
            back[z, y, m] = value
        elif OUT_HOPS == 2 and h == 0 and dz == 0:
            omid[0, dy, z, near] = value
        elif OUT_HOPS == 2 and h == 1 and dy == 0:
            omid[1, dz, y, near] = value
        else:
            made[dz, dy, m] = value

    def gram_stage(c):
        all_of(held.at[after, :, pl.ds(c * count, count)], in2_r.at[c])
        first = lax.broadcasted_iota(jnp.int32, (side, 2 * side), 1) < side

        @pl.loop(0, pairs // 2)
        def _(q):
            for h in (0, 1):
                p = h * (pairs // 2) + q
                for at in (0, 1):
                    near = c * half + 2 * q + at
                    m = c * count + h * half + 2 * q + at
                    for i in range(RING * RING):
                        xs[c, p, pl.ds(at * side + i * share, share), :] = rows_of(h, i, m, near)
            for h in (0, 1):
                p = h * (pairs // 2) + q
                x = xs[c, p]
                both = mul_t(x, x)
                mine[c, p] = jnp.where(first, both[:side], both[side:])

        for p in range(pairs):
            @pl.when(worker(c, p) != col)
            def _():
                gram_send(c, p).start()

    def works(c):
        return lax.rem(col, workers) == c % workers

    def transform_stage(c):
        @pl.when(works(c))
        def _():
            place = col // workers
            all_of(theirs.at[c, pl.ds(1, cols - 1)], rs_r.at[c])
            one = mine[c, place]
            for k in range(1, cols):
                one = one + theirs[c, k]
            fac[c, place] = transform(one, side)
            for k in range(1, cols):
                fac_send(c, place, k).start()

    def apply_stage(c):
        @pl.when(works(c))
        def _():
            all_of(fac.at[c, pl.ds(0, pairs - 1)], ag_r.at[c])

        @pl.when(jnp.logical_not(works(c)))
        def _():
            all_of(fac.at[c], ag_r.at[c])

        @pl.loop(0, pairs // 2)
        def _(q):
            for h in (0, 1):
                p = h * (pairs // 2) + q
                obuf[h] = mul(spread(fac[c, p], side), xs[c, p])
            for h in (0, 1):
                for at in (0, 1):
                    near = c * half + 2 * q + at
                    m = c * count + h * half + 2 * q + at
                    for i in range(RING * RING):
                        keep_rows(h, i, m, near, obuf[h, pl.ds(at * side + i * share, share), :])

        if OUT_HOPS == 2:
            for k in order:
                for h in (0, 1):
                    out1(c, h, k).start()
                    out3(c, h, k).start()
        else:
            for dz, dy in FAR:
                out(c, dz, dy).start()

    def forward_in(c):
        all_of(mid.at[:, after, :, pl.ds(c * half, half)], in1_r.at[c])
        for k in order:
            for h in (0, 1):
                in2(c, h, k).start()
                in3(c, h, k).start()

    def forward_out(c):
        if OUT_HOPS == 2:
            all_of(omid.at[:, after, after, pl.ds(c * half, half)], o1_r.at[c])
            for k in order:
                for h in (0, 1):
                    out2(c, h, k).start()

    stages = {
        "M": momentum_stage, "B": meet, "S": start_in1, "I": forward_in, "G": gram_stage,
        "T": transform_stage, "A": apply_stage, "O": forward_out,
    }
    for event in SCHEDULE:
        stages[event[0]](int(event[1:]))

    if OUT_HOPS == 2:
        all_of(back.at[0, after], end_r.at[0])
        all_of(back.at[after], end_r.at[1])
        all_of(made.at[after, after], sent.at[3])
        all_of(made.at[0, after], sent.at[4])
        all_of(made.at[after], sent.at[5])
    else:
        all_of(back.at[0, after], end_r.at[0])
        all_of(back.at[after], end_r.at[1])
        all_of(made.at[0, after], sent.at[3])
        all_of(made.at[after], sent.at[4])
    all_of(mom.at[after], sent.at[0])
    all_of(mom.at[after, after], sent.at[1])
    all_of(mom.at[0, after], sent.at[2])
    all_of(theirs.at[pl.ds(0, 2), pl.ds(1, cols - 1)], sent.at[6])
    all_of(theirs.at[pl.ds(0, 2), pl.ds(1, cols - 1)], sent.at[7])


FAR = [(2, 2), (2, 3), (3, 2), (2, 1), (1, 2), (2, 0), (0, 2), (3, 1), (1, 3), (3, 3), (1, 1), (3, 0), (0, 3), (1, 0), (0, 1)]


def exchange_and_iterate(grad, moment, cols):
    every, share, width = grad.shape
    mats = every // (RING * RING)
    side = RING * RING * share
    count = mats // CHUNKS
    pairs = count // 2
    f32, dma = jnp.float32, pltpu.SemaphoreType.DMA
    shape = (RING, RING, mats, share, width)
    halves = (2, RING, RING, mats // 2, share, width)
    whole = pl.BlockSpec(memory_space=pltpu.VMEM)
    back, mom = pl.pallas_call(
        functools.partial(kernel, cols),
        out_shape=[jax.ShapeDtypeStruct(shape, f32)] * 2,
        in_specs=[pl.BlockSpec(memory_space=pltpu.HBM)] * 2,
        out_specs=[whole, whole],
        scratch_shapes=[
            pltpu.VMEM(shape, f32),
            pltpu.VMEM(halves, f32),
            pltpu.VMEM(shape, f32),
            pltpu.VMEM(shape, f32),
            pltpu.VMEM(halves, f32),
            pltpu.VMEM((CHUNKS, pairs, 2 * side, width), f32),
            pltpu.VMEM((2, 2 * side, width), f32),
            pltpu.VMEM((CHUNKS, pairs, side, 2 * side), f32),
            pltpu.VMEM((CHUNKS, cols, side, 2 * side), f32),
            pltpu.VMEM((CHUNKS, pairs, side, 2 * side), f32),
            dma((2, CHUNKS)), dma((CHUNKS,)), dma((CHUNKS,)), dma((CHUNKS,)), dma((2,)),
            dma((CHUNKS,)), dma((CHUNKS,)), dma((8,)),
        ],
        compiler_params=pltpu.CompilerParams(
            collective_id=0, has_side_effects=True, vmem_limit_bytes=40 * 2**20
        ),
        name="exchange_and_iterate",
    )(*(pltpu.with_memory_space_constraint(v.reshape(shape), pltpu.HBM) for v in (grad, moment)))
    return back.reshape(grad.shape), mom.reshape(grad.shape)


FINAL = 8


def finish_kernel(weight, back, mom, new_weight, new_mom, made, sems):
    step = weight.shape[0] // FINAL
    whole = pltpu.make_async_copy(mom, new_mom, sems.at[FINAL])
    whole.start()

    def put(i):
        at = pl.ds(i * step, step)
        return pltpu.make_async_copy(made.at[at], new_weight.at[at], sems.at[i])

    @pl.loop(0, FINAL)
    def _(i):
        at = pl.ds(i * step, step)
        made[at] = weight[at] - learn_rate * back[at]
        put(i).start()

    @pl.loop(0, FINAL)
    def _(i):
        put(i).wait()
    whole.wait()


def finish(weight, back, mom):
    here = pl.BlockSpec(memory_space=pltpu.VMEM)
    out = pl.BlockSpec(memory_space=pl.ANY)
    shape = jax.ShapeDtypeStruct(weight.shape, jnp.float32)
    return pl.pallas_call(
        finish_kernel,
        out_shape=[shape, shape],
        in_specs=[here] * 3,
        out_specs=[out, out],
        scratch_shapes=[
            pltpu.VMEM(weight.shape, jnp.float32), pltpu.SemaphoreType.DMA((FINAL + 1,)),
        ],
        compiler_params=pltpu.CompilerParams(vmem_limit_bytes=16 * 2**20),
        name="finish",
    )(weight, back, mom)


def solution(mesh):
    cols = mesh.shape["cols"]

    def on_device(grad_stack, moment_stack, weight_stack):
        back, new_momentum = exchange_and_iterate(grad_stack, moment_stack, cols)
        return tuple(finish(weight_stack, back, new_momentum))

    placed = P(None, "rows", "cols")
    return jax.shard_map(
        on_device,
        mesh=mesh,
        in_specs=(placed, placed, placed),
        out_specs=(placed, placed),
        check_vma=False,
    )
```

```python
import functools

import jax
import jax.numpy as jnp
from jax import lax
from jax.experimental import pallas as pl
from jax.experimental.pallas import tpu as pltpu
from jax.sharding import PartitionSpec as P

ITERS = 5
RING = 4
CHUNKS = 8
SCHEDULE = (
    "M1", "B0", "S1", "M5", "M0", "M7", "M4", "S0", "S7", "S5", "I1", "M6", "I0", "I7",
    "I5", "G1", "M2", "S2", "G0", "S4", "M3", "S6", "S3", "G7", "G5", "I2", "T1", "T0",
    "I4", "T7", "I6", "T5", "I3", "A1", "G2", "A0", "G4", "A7", "G6", "G3", "A5", "O1",
    "T2", "O0", "T4", "O7", "T3", "T6", "O5", "A2", "A4", "A6", "A3", "O2", "O4", "O6",
    "O3",
)

hold_rate = 0.95
learn_rate = 1.0

MESH = pl.DeviceIdType.MESH


def mul(a, b):
    return lax.dot_general(
        a, b, (((1,), (0,)), ((), ())),
        precision=lax.Precision.HIGHEST, preferred_element_type=jnp.float32,
    )


def mul_t(a, b):
    return lax.dot_general(
        a, b, (((1,), (1,)), ((), ())),
        precision=lax.Precision.HIGHEST, preferred_element_type=jnp.float32,
    )


def spread(packed, side):
    first = lax.broadcasted_iota(jnp.int32, (side, 2 * side), 1) < side
    return jnp.concatenate(
        [
            jnp.where(first, packed, jnp.zeros_like(packed)),
            jnp.where(first, jnp.zeros_like(packed), packed),
        ], axis=0,
    )


def parts(x):
    high = x.astype(jnp.bfloat16)
    rest = x - high.astype(jnp.float32)
    mid = rest.astype(jnp.bfloat16)
    low = (rest - mid.astype(jnp.float32)).astype(jnp.bfloat16)
    return high, mid, low


def right(x, side):
    high, mid, low = (spread(part, side) for part in parts(x))
    both = jnp.concatenate(
        [jnp.concatenate([high, mid], axis=1), jnp.concatenate([mid, high], axis=1)], axis=0
    )
    return both, jnp.concatenate([low, high], axis=0)


def times(x, factors):
    both, rest = factors
    wide = rest.shape[1]
    high, mid, low = parts(x)

    def dot(a, b):
        return jnp.dot(a, b, preferred_element_type=jnp.float32)

    large = dot(jnp.concatenate([high, mid], axis=1), both)
    small = dot(jnp.concatenate([high, low], axis=1), rest)
    return large[:, :wide] + (large[:, wide:] + small)


def transform(packed, side):
    wide = 2 * side
    row = lax.broadcasted_iota(jnp.int32, (side, wide), 0)
    lane = lax.broadcasted_iota(jnp.int32, (side, wide), 1)
    first = lane < side
    scales = [
        lax.rsqrt(
            jnp.sum(
                jnp.sum(jnp.where(lane == row + at, packed, 0.0), axis=1, keepdims=True),
                axis=0, keepdims=True,
            ) + 1e-06
        )
        for at in (0, side)
    ]
    scale = jnp.where(first, scales[0], scales[1])
    gram = packed * scale * scale
    eye = jnp.where((lane == row) | (lane == row + side), 3.4445, 0.0)
    total = None
    for step in range(ITERS):
        grams = right(gram, side)
        factor = eye + (-4.775 * gram + 2.0315 * times(gram, grams))
        if step == ITERS - 1:
            total = times(factor, right(total, side))
            break
        inner = times(factor, grams)
        factors = right(factor, side)
        if total is None:
            gram, total = times(inner, factors), factor
        else:
            pair = times(jnp.concatenate([inner, total], axis=0), factors)
            gram, total = pair[:side], pair[side:]
    return total * scale


def kernel(
    cols, grad, moment, back, mom, old, mid, held, made, omid, xs, obuf, mine, theirs, fac,
    load_sem, in1_r, in2_r, o1_r, end_r, rs_r, ag_r, sent,
):
    me, col = lax.axis_index("rows"), lax.axis_index("cols")
    z, y = me // RING, lax.rem(me, RING)
    mats, share, width = mom.shape[2:]
    side = RING * RING * share
    count = mats // CHUNKS
    half = count // 2
    pairs = count // 2
    workers = cols // pairs
    others = range(1, RING)
    order = (2, 1, 3)
    after = pl.ds(1, RING - 1)

    def up(at, k):
        return lax.rem(at + k, RING)

    def down(at, k):
        return lax.rem(at + RING - k, RING)

    def along(h, at):
        return (z * RING + at, col) if h == 0 else (at * RING + y, col)

    def col_peer(k):
        return lax.rem(col + k, cols)

    def all_of(ref, sem):
        pltpu.make_async_copy(ref, ref, sem).wait()

    def remote(src, dst, send, recv, to):
        return pltpu.make_async_remote_copy(
            src_ref=src, dst_ref=dst, send_sem=send, recv_sem=recv,
            device_id=to, device_id_type=MESH,
        )

    barrier = pltpu.get_barrier_semaphore()
    for k in others:
        for h in (0, 1):
            pl.semaphore_signal(
                barrier, inc=1, device_id=along(h, up((y, z)[h], k)), device_id_type=MESH
            )
    for k in range(1, cols):
        pl.semaphore_signal(barrier, inc=1, device_id=(me, col_peer(k)), device_id_type=MESH)

    def load(c):
        at = pl.ds(c * count, count)
        return [
            pltpu.make_async_copy(src.at[:, :, at], dst.at[:, :, at], load_sem.at[n, c])
            for n, (src, dst) in enumerate(((grad, mom), (moment, old)))
        ]

    loads = [int(event[1:]) for event in SCHEDULE if event[0] == "M"]

    def start_loads(some):
        for c in some:
            for copy in load(c):
                copy.start()

    start_loads(loads[:2])

    def meet(_):
        pl.semaphore_wait(barrier, 2 * (RING - 1) + cols - 1)

    def of(h, c):
        return pl.ds(c * count + h * half, half), pl.ds(c * half, half)

    def momentum_stage(c):
        for copy in load(c):
            copy.wait()
        if c == loads[0]:
            start_loads(loads[2:])

        @pl.loop(0, RING * RING)
        def _(i):
            at = (i // RING, lax.rem(i, RING), pl.ds(c * count, count))
            mom[at] = hold_rate * old[at] + mom[at]

        for h in (0, 1):
            at, near = of(h, c)
            for k in range(RING):
                mid[h, 0, k, near] = mom[k, y, at] if h == 0 else mom[z, k, at]

    def in1(c, h, k):
        at, near = of(h, c)
        to = up((y, z)[h], k)
        src = mom.at[:, to, at] if h == 0 else mom.at[to, :, at]
        return remote(src, mid.at[h, k, :, near], sent.at[0], in1_r.at[c], along(h, to))

    def in2(c, h, k):
        at, near = of(h, c)
        to = up((z, y)[h], k)
        dst = held.at[k, :, at] if h == 0 else held.at[:, k, at]
        return remote(mid.at[h, :, to, near], dst, sent.at[1], in2_r.at[c], along(1 - h, to))

    def out1(c, h, k):
        at, near = of(h, c)
        to = down((z, y)[h], k)
        src, dst = (
            (made.at[k, :, at], omid.at[0, :, z, near]) if h == 0
            else (made.at[:, k, at], omid.at[1, :, y, near])
        )
        return remote(src, dst, sent.at[2], o1_r.at[c], along(1 - h, to))

    def out2(c, h, k):
        at, near = of(h, c)
        to = down((y, z)[h], k)
        dst = back.at[:, y, at] if h == 0 else back.at[z, :, at]
        return remote(omid.at[h, k, :, near], dst, sent.at[3], end_r, along(h, to))

    def worker(c, p):
        return workers * p + c % workers

    def gram_send(c, p):
        to = worker(c, p)
        k = lax.rem(col + cols - to, cols)
        return remote(mine.at[c, p], theirs.at[c, k], sent.at[4], rs_r.at[c], (me, to))

    def fac_send(c, p, k):
        return remote(fac.at[c, p], fac.at[c, p], sent.at[5], ag_r.at[c], (me, col_peer(k)))

    def start_in1(c):
        for k in order:
            for h in (0, 1):
                in1(c, h, k).start()

    def rows_of(h, i, m, near):
        dz, dy = i // RING, i % RING
        if i == 0:
            return mom[z, y, m]
        if h == 0 and dz == 0:
            return mid[0, dy, z, near]
        if h == 1 and dy == 0:
            return mid[1, dz, y, near]
        return held[dz, dy, m]

    def keep_rows(h, i, m, near, value):
        dz, dy = i // RING, i % RING
        if i == 0:
            back[z, y, m] = value
        elif h == 0 and dz == 0:
            omid[0, dy, z, near] = value
        elif h == 1 and dy == 0:
            omid[1, dz, y, near] = value
        else:
            made[dz, dy, m] = value

    def gram_stage(c):
        all_of(held.at[after, :, pl.ds(c * count, count)], in2_r.at[c])
        first = lax.broadcasted_iota(jnp.int32, (side, 2 * side), 1) < side

        @pl.loop(0, pairs // 2)
        def _(q):
            for h in (0, 1):
                p = h * (pairs // 2) + q
                for at in (0, 1):
                    near = c * half + 2 * q + at
                    m = c * count + h * half + 2 * q + at
                    for i in range(RING * RING):
                        xs[c, p, pl.ds(at * side + i * share, share), :] = rows_of(h, i, m, near)
            for h in (0, 1):
                p = h * (pairs // 2) + q
                x = xs[c, p]
                both = mul_t(x, x)
                mine[c, p] = jnp.where(first, both[:side], both[side:])

        for p in range(pairs):
            @pl.when(worker(c, p) != col)
            def _():
                gram_send(c, p).start()

    def works(c):
        return lax.rem(col, workers) == c % workers

    def transform_stage(c):
        @pl.when(works(c))
        def _():
            place = col // workers
            all_of(theirs.at[c, pl.ds(1, cols - 1)], rs_r.at[c])
            one = mine[c, place]
            for k in range(1, cols):
                one = one + theirs[c, k]
            fac[c, place] = transform(one, side)
            for k in range(1, cols):
                fac_send(c, place, k).start()

    def apply_stage(c):
        @pl.when(works(c))
        def _():
            all_of(fac.at[c, pl.ds(0, pairs - 1)], ag_r.at[c])

        @pl.when(jnp.logical_not(works(c)))
        def _():
            all_of(fac.at[c], ag_r.at[c])

        @pl.loop(0, pairs // 2)
        def _(q):
            for h in (0, 1):
                p = h * (pairs // 2) + q
                obuf[h] = mul(spread(fac[c, p], side), xs[c, p])
            for h in (0, 1):
                for at in (0, 1):
                    near = c * half + 2 * q + at
                    m = c * count + h * half + 2 * q + at
                    for i in range(RING * RING):
                        keep_rows(h, i, m, near, obuf[h, pl.ds(at * side + i * share, share), :])

        for k in order:
            for h in (0, 1):
                out1(c, h, k).start()

    def forward_in(c):
        all_of(mid.at[:, after, :, pl.ds(c * half, half)], in1_r.at[c])
        for k in order:
            for h in (0, 1):
                in2(c, h, k).start()

    def forward_out(c):
        all_of(omid.at[:, :, after, pl.ds(c * half, half)], o1_r.at[c])
        for k in order:
            for h in (0, 1):
                out2(c, h, k).start()
        for h in (0, 1):
            at, near = of(h, c)
            for k in others:
                here = up((z, y)[h], k)
                if h == 0:
                    back[here, y, at] = omid[0, 0, here, near]
                else:
                    back[z, here, at] = omid[1, 0, here, near]

    stages = {
        "M": momentum_stage, "B": meet, "S": start_in1, "I": forward_in, "G": gram_stage,
        "T": transform_stage, "A": apply_stage, "O": forward_out,
    }
    for event in SCHEDULE:
        stages[event[0]](int(event[1:]))

    all_of(back.at[after], end_r)
    all_of(mom.at[after], sent.at[0])
    all_of(mom.at[after], sent.at[1])
    all_of(made.at[after], sent.at[2])
    all_of(made.at[after], sent.at[3])
    all_of(theirs.at[pl.ds(0, 2), pl.ds(1, cols - 1)], sent.at[4])
    all_of(theirs.at[pl.ds(0, 2), pl.ds(1, cols - 1)], sent.at[5])


def exchange_and_iterate(grad, moment, cols):
    every, share, width = grad.shape
    mats = every // (RING * RING)
    side = RING * RING * share
    count = mats // CHUNKS
    pairs = count // 2
    f32, dma = jnp.float32, pltpu.SemaphoreType.DMA
    shape = (RING, RING, mats, share, width)
    halves = (2, RING, RING, mats // 2, share, width)
    whole = pl.BlockSpec(memory_space=pltpu.VMEM)
    back, mom = pl.pallas_call(
        functools.partial(kernel, cols),
        out_shape=[jax.ShapeDtypeStruct(shape, f32)] * 2,
        in_specs=[pl.BlockSpec(memory_space=pltpu.HBM)] * 2,
        out_specs=[whole, whole],
        scratch_shapes=[
            pltpu.VMEM(shape, f32),
            pltpu.VMEM(halves, f32),
            pltpu.VMEM(shape, f32),
            pltpu.VMEM(shape, f32),
            pltpu.VMEM(halves, f32),
            pltpu.VMEM((CHUNKS, pairs, 2 * side, width), f32),
            pltpu.VMEM((2, 2 * side, width), f32),
            pltpu.VMEM((CHUNKS, pairs, side, 2 * side), f32),
            pltpu.VMEM((CHUNKS, cols, side, 2 * side), f32),
            pltpu.VMEM((CHUNKS, pairs, side, 2 * side), f32),
            dma((2, CHUNKS)), dma((CHUNKS,)), dma((CHUNKS,)), dma((CHUNKS,)), dma(()),
            dma((CHUNKS,)), dma((CHUNKS,)), dma((6,)),
        ],
        compiler_params=pltpu.CompilerParams(
            collective_id=0, has_side_effects=True, vmem_limit_bytes=40 * 2**20
        ),
        name="exchange_and_iterate",
    )(*(pltpu.with_memory_space_constraint(v.reshape(shape), pltpu.HBM) for v in (grad, moment)))
    return back.reshape(grad.shape), mom.reshape(grad.shape)


FINAL = 8


def finish_kernel(weight, back, mom, new_weight, new_mom, made, sems):
    step = weight.shape[0] // FINAL
    whole = pltpu.make_async_copy(mom, new_mom, sems.at[FINAL])
    whole.start()

    def put(i):
        at = pl.ds(i * step, step)
        return pltpu.make_async_copy(made.at[at], new_weight.at[at], sems.at[i])

    @pl.loop(0, FINAL)
    def _(i):
        at = pl.ds(i * step, step)
        made[at] = weight[at] - learn_rate * back[at]
        put(i).start()

    @pl.loop(0, FINAL)
    def _(i):
        put(i).wait()
    whole.wait()


def finish(weight, back, mom):
    here = pl.BlockSpec(memory_space=pltpu.VMEM)
    out = pl.BlockSpec(memory_space=pl.ANY)
    shape = jax.ShapeDtypeStruct(weight.shape, jnp.float32)
    return pl.pallas_call(
        finish_kernel,
        out_shape=[shape, shape],
        in_specs=[here] * 3,
        out_specs=[out, out],
        scratch_shapes=[
            pltpu.VMEM(weight.shape, jnp.float32), pltpu.SemaphoreType.DMA((FINAL + 1,)),
        ],
        compiler_params=pltpu.CompilerParams(vmem_limit_bytes=16 * 2**20),
        name="finish",
    )(weight, back, mom)


def solution(mesh):
    cols = mesh.shape["cols"]

    def on_device(grad_stack, moment_stack, weight_stack):
        back, new_momentum = exchange_and_iterate(grad_stack, moment_stack, cols)
        return tuple(finish(weight_stack, back, new_momentum))

    placed = P(None, "rows", "cols")
    return jax.shard_map(
        on_device,
        mesh=mesh,
        in_specs=(placed, placed, placed),
        out_specs=(placed, placed),
        check_vma=False,
    )
```

```python
import functools

import jax
import jax.numpy as jnp
from jax import lax
from jax.experimental import pallas as pl
from jax.experimental.pallas import tpu as pltpu
from jax.sharding import PartitionSpec as P

ITERS = 5
RING = 4
CHUNKS = 8
SCHEDULE = (
    "M1", "B0", "S1", "M5", "M0", "M7", "M4", "S0", "S7", "S5", "I1", "M6", "I0", "I7",
    "I5", "G1", "M2", "S2", "G0", "S4", "M3", "S6", "S3", "G7", "G5", "I2", "T1", "T0",
    "I4", "T7", "I6", "T5", "I3", "A1", "G2", "A0", "G4", "A7", "G6", "G3", "A5", "O1",
    "T2", "O0", "T4", "O7", "T3", "T6", "O5", "A2", "A4", "A6", "A3", "O2", "O4", "O6",
    "O3",
)

hold_rate = 0.95
learn_rate = 1.0

MESH = pl.DeviceIdType.MESH


def mul(a, b):
    return lax.dot_general(
        a, b, (((1,), (0,)), ((), ())),
        precision=lax.Precision.HIGHEST, preferred_element_type=jnp.float32,
    )


def mul_t(a, b):
    return lax.dot_general(
        a, b, (((1,), (1,)), ((), ())),
        precision=lax.Precision.HIGHEST, preferred_element_type=jnp.float32,
    )


def spread(packed, side):
    first = lax.broadcasted_iota(jnp.int32, (side, 2 * side), 1) < side
    return jnp.concatenate(
        [
            jnp.where(first, packed, jnp.zeros_like(packed)),
            jnp.where(first, jnp.zeros_like(packed), packed),
        ], axis=0,
    )


def parts(x):
    high = x.astype(jnp.bfloat16)
    rest = x - high.astype(jnp.float32)
    mid = rest.astype(jnp.bfloat16)
    low = (rest - mid.astype(jnp.float32)).astype(jnp.bfloat16)
    return high, mid, low


def right(x, side):
    high, mid, low = (spread(part, side) for part in parts(x))
    both = jnp.concatenate(
        [jnp.concatenate([high, mid], axis=1), jnp.concatenate([mid, high], axis=1)], axis=0
    )
    return both, jnp.concatenate([low, high], axis=0)


def times(x, factors):
    both, rest = factors
    wide = rest.shape[1]
    high, mid, low = parts(x)

    def dot(a, b):
        return jnp.dot(a, b, preferred_element_type=jnp.float32)

    large = dot(jnp.concatenate([high, mid], axis=1), both)
    small = dot(jnp.concatenate([high, low], axis=1), rest)
    return large[:, :wide] + (large[:, wide:] + small)


def transform(packed, side):
    wide = 2 * side
    row = lax.broadcasted_iota(jnp.int32, (side, wide), 0)
    lane = lax.broadcasted_iota(jnp.int32, (side, wide), 1)
    first = lane < side
    scales = [
        lax.rsqrt(
            jnp.sum(
                jnp.sum(jnp.where(lane == row + at, packed, 0.0), axis=1, keepdims=True),
                axis=0, keepdims=True,
            ) + 1e-06
        )
        for at in (0, side)
    ]
    scale = jnp.where(first, scales[0], scales[1])
    gram = packed * scale * scale
    eye = jnp.where((lane == row) | (lane == row + side), 3.4445, 0.0)
    total = None
    for step in range(ITERS):
        grams = right(gram, side)
        factor = eye + (-4.775 * gram + 2.0315 * times(gram, grams))
        if step == ITERS - 1:
            total = times(factor, right(total, side))
            break
        inner = times(factor, grams)
        factors = right(factor, side)
        if total is None:
            gram, total = times(inner, factors), factor
        else:
            pair = times(jnp.concatenate([inner, total], axis=0), factors)
            gram, total = pair[:side], pair[side:]
    return total * scale


def kernel(
    cols, grad, moment, back, mom, old, mid, held, made, omid, xs, obuf, mine, theirs, fac,
    load_sem, in1_r, in2_r, o1_r, end_r, rs_r, ag_r, sent,
):
    me, col = lax.axis_index("rows"), lax.axis_index("cols")
    z, y = me // RING, lax.rem(me, RING)
    mats, share, width = mom.shape[2:]
    side = RING * RING * share
    count = mats // CHUNKS
    half = count // 2
    pairs = count // 2
    workers = cols // pairs
    others = range(1, RING)
    order = (2, 1, 3)
    after = pl.ds(1, RING - 1)

    def up(at, k):
        return lax.rem(at + k, RING)

    def down(at, k):
        return lax.rem(at + RING - k, RING)

    def along(h, at):
        return (z * RING + at, col) if h == 0 else (at * RING + y, col)

    def col_peer(k):
        return lax.rem(col + k, cols)

    def all_of(ref, sem):
        pltpu.make_async_copy(ref, ref, sem).wait()

    def remote(src, dst, send, recv, to):
        return pltpu.make_async_remote_copy(
            src_ref=src, dst_ref=dst, send_sem=send, recv_sem=recv,
            device_id=to, device_id_type=MESH,
        )

    barrier = pltpu.get_barrier_semaphore()
    for k in others:
        for h in (0, 1):
            pl.semaphore_signal(
                barrier, inc=1, device_id=along(h, up((y, z)[h], k)), device_id_type=MESH
            )
    for k in range(1, cols):
        pl.semaphore_signal(barrier, inc=1, device_id=(me, col_peer(k)), device_id_type=MESH)

    def load(c):
        at = pl.ds(c * count, count)
        return [
            pltpu.make_async_copy(src.at[:, :, at], dst.at[:, :, at], load_sem.at[n, c])
            for n, (src, dst) in enumerate(((grad, mom), (moment, old)))
        ]

    loads = [int(event[1:]) for event in SCHEDULE if event[0] == "M"]

    def start_loads(some):
        for c in some:
            for copy in load(c):
                copy.start()

    start_loads(loads[:2])

    def meet(_):
        pl.semaphore_wait(barrier, 2 * (RING - 1) + cols - 1)

    def of(h, c):
        return pl.ds(c * count + h * half, half), pl.ds(c * half, half)

    def momentum_stage(c):
        for copy in load(c):
            copy.wait()
        if c == loads[0]:
            start_loads(loads[2:])

        @pl.loop(0, RING * RING)
        def _(i):
            at = (i // RING, lax.rem(i, RING), pl.ds(c * count, count))
            mom[at] = hold_rate * old[at] + mom[at]

        for h in (0, 1):
            at, near = of(h, c)
            for k in range(RING):
                mid[h, 0, k, near] = mom[k, y, at] if h == 0 else mom[z, k, at]

    def in1(c, h, k):
        at, near = of(h, c)
        to = up((y, z)[h], k)
        src = mom.at[:, to, at] if h == 0 else mom.at[to, :, at]
        return remote(src, mid.at[h, k, :, near], sent.at[0], in1_r.at[c], along(h, to))

    def in2(c, h, k):
        at, near = of(h, c)
        to = up((z, y)[h], k)
        dst = held.at[k, :, at] if h == 0 else held.at[:, k, at]
        return remote(mid.at[h, :, to, near], dst, sent.at[1], in2_r.at[c], along(1 - h, to))

    def out1(c, h, k):
        at, near = of(h, c)
        to = down((z, y)[h], k)
        src, dst = (
            (made.at[k, :, at], omid.at[0, :, z, near]) if h == 0
            else (made.at[:, k, at], omid.at[1, :, y, near])
        )
        return remote(src, dst, sent.at[2], o1_r.at[c], along(1 - h, to))

    def out2(c, h, k):
        at, near = of(h, c)
        to = down((y, z)[h], k)
        dst = back.at[:, y, at] if h == 0 else back.at[z, :, at]
        return remote(omid.at[h, k, :, near], dst, sent.at[3], end_r, along(h, to))

    def worker(c, p):
        return workers * p + (c + 1) % workers

    def gram_send(c, p):
        to = worker(c, p)
        k = lax.rem(col + cols - to, cols)
        return remote(mine.at[c, p], theirs.at[c, k], sent.at[4], rs_r.at[c], (me, to))

    def fac_send(c, p, k):
        return remote(fac.at[c, p], fac.at[c, p], sent.at[5], ag_r.at[c], (me, col_peer(k)))

    def start_in1(c):
        for k in order:
            for h in (0, 1):
                in1(c, h, k).start()

    def rows_of(h, i, m, near):
        dz, dy = i // RING, i % RING
        if i == 0:
            return mom[z, y, m]
        if h == 0 and dz == 0:
            return mid[0, dy, z, near]
        if h == 1 and dy == 0:
            return mid[1, dz, y, near]
        return held[dz, dy, m]

    def keep_rows(h, i, m, near, value):
        dz, dy = i // RING, i % RING
        if i == 0:
            back[z, y, m] = value
        elif h == 0 and dz == 0:
            omid[0, dy, z, near] = value
        elif h == 1 and dy == 0:
            omid[1, dz, y, near] = value
        else:
            made[dz, dy, m] = value

    def gram_stage(c):
        all_of(held.at[after, :, pl.ds(c * count, count)], in2_r.at[c])
        first = lax.broadcasted_iota(jnp.int32, (side, 2 * side), 1) < side

        @pl.loop(0, pairs // 2)
        def _(q):
            for h in (0, 1):
                p = h * (pairs // 2) + q
                for at in (0, 1):
                    near = c * half + 2 * q + at
                    m = c * count + h * half + 2 * q + at
                    for i in range(RING * RING):
                        xs[c, p, pl.ds(at * side + i * share, share), :] = rows_of(h, i, m, near)
            for h in (0, 1):
                p = h * (pairs // 2) + q
                x = xs[c, p]
                both = mul_t(x, x)
                mine[c, p] = jnp.where(first, both[:side], both[side:])

        for p in range(pairs):
            @pl.when(worker(c, p) != col)
            def _():
                gram_send(c, p).start()

    def works(c):
        return lax.rem(col, workers) == (c + 1) % workers

    def transform_stage(c):
        @pl.when(works(c))
        def _():
            place = col // workers
            all_of(theirs.at[c, pl.ds(1, cols - 1)], rs_r.at[c])
            one = mine[c, place]
            for k in range(1, cols):
                one = one + theirs[c, k]
            fac[c, place] = transform(one, side)
            for k in range(1, cols):
                fac_send(c, place, k).start()

    def apply_stage(c):
        @pl.when(works(c))
        def _():
            all_of(fac.at[c, pl.ds(0, pairs - 1)], ag_r.at[c])

        @pl.when(jnp.logical_not(works(c)))
        def _():
            all_of(fac.at[c], ag_r.at[c])

        @pl.loop(0, pairs // 2)
        def _(q):
            for h in (0, 1):
                p = h * (pairs // 2) + q
                obuf[h] = mul(spread(fac[c, p], side), xs[c, p])
            for h in (0, 1):
                for at in (0, 1):
                    near = c * half + 2 * q + at
                    m = c * count + h * half + 2 * q + at
                    for i in range(RING * RING):
                        keep_rows(h, i, m, near, obuf[h, pl.ds(at * side + i * share, share), :])

        for k in order:
            for h in (0, 1):
                out1(c, h, k).start()

    def forward_in(c):
        all_of(mid.at[:, after, :, pl.ds(c * half, half)], in1_r.at[c])
        for k in order:
            for h in (0, 1):
                in2(c, h, k).start()

    def forward_out(c):
        all_of(omid.at[:, :, after, pl.ds(c * half, half)], o1_r.at[c])
        for k in order:
            for h in (0, 1):
                out2(c, h, k).start()
        for h in (0, 1):
            at, near = of(h, c)
            for k in others:
                here = up((z, y)[h], k)
                if h == 0:
                    back[here, y, at] = omid[0, 0, here, near]
                else:
                    back[z, here, at] = omid[1, 0, here, near]

    stages = {
        "M": momentum_stage, "B": meet, "S": start_in1, "I": forward_in, "G": gram_stage,
        "T": transform_stage, "A": apply_stage, "O": forward_out,
    }
    for event in SCHEDULE:
        stages[event[0]](int(event[1:]))

    all_of(back.at[after], end_r)
    all_of(mom.at[after], sent.at[0])
    all_of(mom.at[after], sent.at[1])
    all_of(made.at[after], sent.at[2])
    all_of(made.at[after], sent.at[3])
    all_of(theirs.at[pl.ds(0, 2), pl.ds(1, cols - 1)], sent.at[4])
    all_of(theirs.at[pl.ds(0, 2), pl.ds(1, cols - 1)], sent.at[5])


def exchange_and_iterate(grad, moment, cols):
    every, share, width = grad.shape
    mats = every // (RING * RING)
    side = RING * RING * share
    count = mats // CHUNKS
    pairs = count // 2
    f32, dma = jnp.float32, pltpu.SemaphoreType.DMA
    shape = (RING, RING, mats, share, width)
    halves = (2, RING, RING, mats // 2, share, width)
    whole = pl.BlockSpec(memory_space=pltpu.VMEM)
    back, mom = pl.pallas_call(
        functools.partial(kernel, cols),
        out_shape=[jax.ShapeDtypeStruct(shape, f32)] * 2,
        in_specs=[pl.BlockSpec(memory_space=pltpu.HBM)] * 2,
        out_specs=[whole, whole],
        scratch_shapes=[
            pltpu.VMEM(shape, f32),
            pltpu.VMEM(halves, f32),
            pltpu.VMEM(shape, f32),
            pltpu.VMEM(shape, f32),
            pltpu.VMEM(halves, f32),
            pltpu.VMEM((CHUNKS, pairs, 2 * side, width), f32),
            pltpu.VMEM((2, 2 * side, width), f32),
            pltpu.VMEM((CHUNKS, pairs, side, 2 * side), f32),
            pltpu.VMEM((CHUNKS, cols, side, 2 * side), f32),
            pltpu.VMEM((CHUNKS, pairs, side, 2 * side), f32),
            dma((2, CHUNKS)), dma((CHUNKS,)), dma((CHUNKS,)), dma((CHUNKS,)), dma(()),
            dma((CHUNKS,)), dma((CHUNKS,)), dma((6,)),
        ],
        compiler_params=pltpu.CompilerParams(
            collective_id=0, has_side_effects=True, vmem_limit_bytes=40 * 2**20
        ),
        name="exchange_and_iterate",
    )(*(pltpu.with_memory_space_constraint(v.reshape(shape), pltpu.HBM) for v in (grad, moment)))
    return back.reshape(grad.shape), mom.reshape(grad.shape)


FINAL = 4


def finish_kernel(weight, back, mom, new_weight, new_mom, made, sems):
    step = weight.shape[0] // FINAL
    whole = pltpu.make_async_copy(mom, new_mom, sems.at[FINAL])
    whole.start()

    def put(i):
        at = pl.ds(i * step, step)
        return pltpu.make_async_copy(made.at[at], new_weight.at[at], sems.at[i])

    @pl.loop(0, FINAL)
    def _(i):
        at = pl.ds(i * step, step)
        made[at] = weight[at] - learn_rate * back[at]
        put(i).start()

    @pl.loop(0, FINAL)
    def _(i):
        put(i).wait()
    whole.wait()


def finish(weight, back, mom):
    here = pl.BlockSpec(memory_space=pltpu.VMEM)
    out = pl.BlockSpec(memory_space=pl.ANY)
    shape = jax.ShapeDtypeStruct(weight.shape, jnp.float32)
    return pl.pallas_call(
        finish_kernel,
        out_shape=[shape, shape],
        in_specs=[here] * 3,
        out_specs=[out, out],
        scratch_shapes=[
            pltpu.VMEM(weight.shape, jnp.float32), pltpu.SemaphoreType.DMA((FINAL + 1,)),
        ],
        compiler_params=pltpu.CompilerParams(vmem_limit_bytes=16 * 2**20),
        name="finish",
    )(weight, back, mom)


def solution(mesh):
    cols = mesh.shape["cols"]

    def on_device(grad_stack, moment_stack, weight_stack):
        back, new_momentum = exchange_and_iterate(grad_stack, moment_stack, cols)
        return tuple(finish(weight_stack, back, new_momentum))

    placed = P(None, "rows", "cols")
    return jax.shard_map(
        on_device,
        mesh=mesh,
        in_specs=(placed, placed, placed),
        out_specs=(placed, placed),
        check_vma=False,
    )
```

```python
import functools

import jax
import jax.numpy as jnp
from jax import lax
from jax.experimental import pallas as pl
from jax.experimental.pallas import tpu as pltpu
from jax.sharding import PartitionSpec as P

ITERS = 5
RING = 4
CHUNKS = 8
SCHEDULE = (
    "M1", "B0", "S1", "M5", "M0", "M7", "M4", "S0", "S7", "S5", "I1", "M6", "I0", "I7",
    "I5", "G1", "M2", "S2", "G0", "S4", "M3", "S6", "S3", "G7", "G5", "I2", "T1", "T0",
    "I4", "T7", "I6", "T5", "I3", "A1", "G2", "A0", "G4", "A7", "G6", "G3", "A5", "O1",
    "T2", "O0", "T4", "O7", "T3", "T6", "O5", "A2", "A4", "A6", "A3", "O2", "O4", "O6",
    "O3",
)

hold_rate = 0.95
learn_rate = 1.0

MESH = pl.DeviceIdType.MESH


def mul(a, b):
    return lax.dot_general(
        a, b, (((1,), (0,)), ((), ())),
        precision=lax.Precision.HIGHEST, preferred_element_type=jnp.float32,
    )


def mul_t(a, b):
    return lax.dot_general(
        a, b, (((1,), (1,)), ((), ())),
        precision=lax.Precision.HIGHEST, preferred_element_type=jnp.float32,
    )


def spread(packed, side):
    first = lax.broadcasted_iota(jnp.int32, (side, 2 * side), 1) < side
    return jnp.concatenate(
        [
            jnp.where(first, packed, jnp.zeros_like(packed)),
            jnp.where(first, jnp.zeros_like(packed), packed),
        ], axis=0,
    )


def parts(x):
    high = x.astype(jnp.bfloat16)
    rest = x - high.astype(jnp.float32)
    mid = rest.astype(jnp.bfloat16)
    low = (rest - mid.astype(jnp.float32)).astype(jnp.bfloat16)
    return high, mid, low


def right(x, side):
    high, mid, low = (spread(part, side) for part in parts(x))
    both = jnp.concatenate(
        [jnp.concatenate([high, mid], axis=1), jnp.concatenate([mid, high], axis=1)], axis=0
    )
    return both, jnp.concatenate([low, high], axis=0)


def times(x, factors):
    both, rest = factors
    wide = rest.shape[1]
    high, mid, low = parts(x)

    def dot(a, b):
        return jnp.dot(a, b, preferred_element_type=jnp.float32)

    large = dot(jnp.concatenate([high, mid], axis=1), both)
    small = dot(jnp.concatenate([high, low], axis=1), rest)
    return large[:, :wide] + (large[:, wide:] + small)


def transform(packed, side):
    wide = 2 * side
    row = lax.broadcasted_iota(jnp.int32, (side, wide), 0)
    lane = lax.broadcasted_iota(jnp.int32, (side, wide), 1)
    first = lane < side
    scales = [
        lax.rsqrt(
            jnp.sum(
                jnp.sum(jnp.where(lane == row + at, packed, 0.0), axis=1, keepdims=True),
                axis=0, keepdims=True,
            ) + 1e-06
        )
        for at in (0, side)
    ]
    scale = jnp.where(first, scales[0], scales[1])
    gram = packed * scale * scale
    eye = jnp.where((lane == row) | (lane == row + side), 3.4445, 0.0)
    total = None
    for step in range(ITERS):
        grams = right(gram, side)
        factor = eye + (-4.775 * gram + 2.0315 * times(gram, grams))
        if step == ITERS - 1:
            total = times(factor, right(total, side))
            break
        inner = times(factor, grams)
        factors = right(factor, side)
        if total is None:
            gram, total = times(inner, factors), factor
        else:
            pair = times(jnp.concatenate([inner, total], axis=0), factors)
            gram, total = pair[:side], pair[side:]
    return total * scale


def kernel(
    cols, grad, moment, back, mom, old, mid, held, made, omid, xs, obuf, mine, theirs, fac,
    load_sem, in1_r, in2_r, o1_r, end_r, rs_r, ag_r, sent,
):
    me, col = lax.axis_index("rows"), lax.axis_index("cols")
    z, y = me // RING, lax.rem(me, RING)
    mats, share, width = mom.shape[2:]
    side = RING * RING * share
    count = mats // CHUNKS
    half = count // 2
    pairs = count // 2
    workers = cols // pairs
    others = range(1, RING)
    order = (2, 1, 3)
    after = pl.ds(1, RING - 1)

    def up(at, k):
        return lax.rem(at + k, RING)

    def down(at, k):
        return lax.rem(at + RING - k, RING)

    def along(h, at):
        return (z * RING + at, col) if h == 0 else (at * RING + y, col)

    def col_peer(k):
        return lax.rem(col + k, cols)

    def all_of(ref, sem):
        pltpu.make_async_copy(ref, ref, sem).wait()

    def remote(src, dst, send, recv, to):
        return pltpu.make_async_remote_copy(
            src_ref=src, dst_ref=dst, send_sem=send, recv_sem=recv,
            device_id=to, device_id_type=MESH,
        )

    barrier = pltpu.get_barrier_semaphore()
    for k in others:
        for h in (0, 1):
            pl.semaphore_signal(
                barrier, inc=1, device_id=along(h, up((y, z)[h], k)), device_id_type=MESH
            )
    for k in range(1, cols):
        pl.semaphore_signal(barrier, inc=1, device_id=(me, col_peer(k)), device_id_type=MESH)

    def load(c):
        at = pl.ds(c * count, count)
        return [
            pltpu.make_async_copy(src.at[:, :, at], dst.at[:, :, at], load_sem.at[n, c])
            for n, (src, dst) in enumerate(((grad, mom), (moment, old)))
        ]

    loads = [int(event[1:]) for event in SCHEDULE if event[0] == "M"]

    def start_loads(some):
        for c in some:
            for copy in load(c):
                copy.start()

    start_loads(loads[:2])

    def meet(_):
        pl.semaphore_wait(barrier, 2 * (RING - 1) + cols - 1)

    def of(h, c):
        return pl.ds(c * count + h * half, half), pl.ds(c * half, half)

    def momentum_stage(c):
        for copy in load(c):
            copy.wait()
        if c == loads[0]:
            start_loads(loads[2:])

        @pl.loop(0, RING * RING)
        def _(i):
            at = (i // RING, lax.rem(i, RING), pl.ds(c * count, count))
            mom[at] = hold_rate * old[at] + mom[at]

        for h in (0, 1):
            at, near = of(h, c)
            for k in range(RING):
                mid[h, 0, k, near] = mom[k, y, at] if h == 0 else mom[z, k, at]

    def in1(c, h, k):
        at, near = of(h, c)
        to = up((y, z)[h], k)
        src = mom.at[:, to, at] if h == 0 else mom.at[to, :, at]
        return remote(src, mid.at[h, k, :, near], sent.at[0], in1_r.at[c], along(h, to))

    def in2(c, h, k):
        at, near = of(h, c)
        to = up((z, y)[h], k)
        dst = held.at[k, :, at] if h == 0 else held.at[:, k, at]
        return remote(mid.at[h, :, to, near], dst, sent.at[1], in2_r.at[c], along(1 - h, to))

    def out1(c, h, k):
        at, near = of(h, c)
        to = down((z, y)[h], k)
        src, dst = (
            (made.at[k, :, at], omid.at[0, :, z, near]) if h == 0
            else (made.at[:, k, at], omid.at[1, :, y, near])
        )
        return remote(src, dst, sent.at[2], o1_r.at[c], along(1 - h, to))

    def out2(c, h, k):
        at, near = of(h, c)
        to = down((y, z)[h], k)
        dst = back.at[:, y, at] if h == 0 else back.at[z, :, at]
        return remote(omid.at[h, k, :, near], dst, sent.at[3], end_r, along(h, to))

    def worker(c, p):
        return workers * p + (c + 1) % workers

    def gram_send(c, p):
        to = worker(c, p)
        k = lax.rem(col + cols - to, cols)
        return remote(mine.at[c, p], theirs.at[c, k], sent.at[4], rs_r.at[c], (me, to))

    def fac_send(c, p, k):
        return remote(fac.at[c, p], fac.at[c, p], sent.at[5], ag_r.at[c], (me, col_peer(k)))

    def start_in1(c):
        for k in order:
            for h in (0, 1):
                in1(c, h, k).start()

    def rows_of(h, i, m, near):
        dz, dy = i // RING, i % RING
        if i == 0:
            return mom[z, y, m]
        if h == 0 and dz == 0:
            return mid[0, dy, z, near]
        if h == 1 and dy == 0:
            return mid[1, dz, y, near]
        return held[dz, dy, m]

    def keep_rows(h, i, m, near, value):
        dz, dy = i // RING, i % RING
        if i == 0:
            back[z, y, m] = value
        elif h == 0 and dz == 0:
            omid[0, dy, z, near] = value
        elif h == 1 and dy == 0:
            omid[1, dz, y, near] = value
        else:
            made[dz, dy, m] = value

    def gram_stage(c):
        all_of(held.at[after, :, pl.ds(c * count, count)], in2_r.at[c])
        first = lax.broadcasted_iota(jnp.int32, (side, 2 * side), 1) < side

        @pl.loop(0, pairs // 2)
        def _(q):
            for h in (0, 1):
                p = h * (pairs // 2) + q
                for at in (0, 1):
                    near = c * half + 2 * q + at
                    m = c * count + h * half + 2 * q + at
                    for i in range(RING * RING):
                        xs[c, p, pl.ds(at * side + i * share, share), :] = rows_of(h, i, m, near)
            for h in (0, 1):
                p = h * (pairs // 2) + q
                x = xs[c, p]
                both = mul_t(x, x)
                mine[c, p] = jnp.where(first, both[:side], both[side:])

        for p in range(pairs):
            @pl.when(worker(c, p) != col)
            def _():
                gram_send(c, p).start()

    def works(c):
        return lax.rem(col, workers) == (c + 1) % workers

    def transform_stage(c):
        @pl.when(works(c))
        def _():
            place = col // workers
            all_of(theirs.at[c, pl.ds(1, cols - 1)], rs_r.at[c])
            one = mine[c, place]
            for k in range(1, cols):
                one = one + theirs[c, k]
            fac[c, place] = transform(one, side)
            for k in sorted(range(1, cols), key=lambda k: abs(k - cols // 2)):
                fac_send(c, place, k).start()

    def apply_stage(c):
        @pl.when(works(c))
        def _():
            all_of(fac.at[c, pl.ds(0, pairs - 1)], ag_r.at[c])

        @pl.when(jnp.logical_not(works(c)))
        def _():
            all_of(fac.at[c], ag_r.at[c])

        @pl.loop(0, pairs // 2)
        def _(q):
            for h in (0, 1):
                p = h * (pairs // 2) + q
                obuf[h] = mul(spread(fac[c, p], side), xs[c, p])
            for h in (0, 1):
                for at in (0, 1):
                    near = c * half + 2 * q + at
                    m = c * count + h * half + 2 * q + at
                    for i in range(RING * RING):
                        keep_rows(h, i, m, near, obuf[h, pl.ds(at * side + i * share, share), :])

        for k in order:
            for h in (0, 1):
                out1(c, h, k).start()

    def forward_in(c):
        all_of(mid.at[:, after, :, pl.ds(c * half, half)], in1_r.at[c])
        for k in order:
            for h in (0, 1):
                in2(c, h, k).start()

    def forward_out(c):
        all_of(omid.at[:, :, after, pl.ds(c * half, half)], o1_r.at[c])
        for k in order:
            for h in (0, 1):
                out2(c, h, k).start()
        for h in (0, 1):
            at, near = of(h, c)
            for k in others:
                here = up((z, y)[h], k)
                if h == 0:
                    back[here, y, at] = omid[0, 0, here, near]
                else:
                    back[z, here, at] = omid[1, 0, here, near]

    stages = {
        "M": momentum_stage, "B": meet, "S": start_in1, "I": forward_in, "G": gram_stage,
        "T": transform_stage, "A": apply_stage, "O": forward_out,
    }
    for event in SCHEDULE:
        stages[event[0]](int(event[1:]))

    all_of(back.at[after], end_r)
    all_of(mom.at[after], sent.at[0])
    all_of(mom.at[after], sent.at[1])
    all_of(made.at[after], sent.at[2])
    all_of(made.at[after], sent.at[3])
    all_of(theirs.at[pl.ds(0, 2), pl.ds(1, cols - 1)], sent.at[4])
    all_of(theirs.at[pl.ds(0, 2), pl.ds(1, cols - 1)], sent.at[5])


def exchange_and_iterate(grad, moment, cols):
    every, share, width = grad.shape
    mats = every // (RING * RING)
    side = RING * RING * share
    count = mats // CHUNKS
    pairs = count // 2
    f32, dma = jnp.float32, pltpu.SemaphoreType.DMA
    shape = (RING, RING, mats, share, width)
    halves = (2, RING, RING, mats // 2, share, width)
    whole = pl.BlockSpec(memory_space=pltpu.VMEM)
    back, mom = pl.pallas_call(
        functools.partial(kernel, cols),
        out_shape=[jax.ShapeDtypeStruct(shape, f32)] * 2,
        in_specs=[pl.BlockSpec(memory_space=pltpu.HBM)] * 2,
        out_specs=[whole, whole],
        scratch_shapes=[
            pltpu.VMEM(shape, f32),
            pltpu.VMEM(halves, f32),
            pltpu.VMEM(shape, f32),
            pltpu.VMEM(shape, f32),
            pltpu.VMEM(halves, f32),
            pltpu.VMEM((CHUNKS, pairs, 2 * side, width), f32),
            pltpu.VMEM((2, 2 * side, width), f32),
            pltpu.VMEM((CHUNKS, pairs, side, 2 * side), f32),
            pltpu.VMEM((CHUNKS, cols, side, 2 * side), f32),
            pltpu.VMEM((CHUNKS, pairs, side, 2 * side), f32),
            dma((2, CHUNKS)), dma((CHUNKS,)), dma((CHUNKS,)), dma((CHUNKS,)), dma(()),
            dma((CHUNKS,)), dma((CHUNKS,)), dma((6,)),
        ],
        compiler_params=pltpu.CompilerParams(
            collective_id=0, has_side_effects=True, vmem_limit_bytes=40 * 2**20
        ),
        name="exchange_and_iterate",
    )(*(pltpu.with_memory_space_constraint(v.reshape(shape), pltpu.HBM) for v in (grad, moment)))
    return back.reshape(grad.shape), mom.reshape(grad.shape)


FINAL = 4


def finish_kernel(weight, back, mom, new_weight, new_mom, made, sems):
    step = weight.shape[0] // FINAL
    whole = pltpu.make_async_copy(mom, new_mom, sems.at[FINAL])
    whole.start()

    def put(i):
        at = pl.ds(i * step, step)
        return pltpu.make_async_copy(made.at[at], new_weight.at[at], sems.at[i])

    @pl.loop(0, FINAL)
    def _(i):
        at = pl.ds(i * step, step)
        made[at] = weight[at] - learn_rate * back[at]
        put(i).start()

    @pl.loop(0, FINAL)
    def _(i):
        put(i).wait()
    whole.wait()


def finish(weight, back, mom):
    here = pl.BlockSpec(memory_space=pltpu.VMEM)
    out = pl.BlockSpec(memory_space=pl.ANY)
    shape = jax.ShapeDtypeStruct(weight.shape, jnp.float32)
    return pl.pallas_call(
        finish_kernel,
        out_shape=[shape, shape],
        in_specs=[here] * 3,
        out_specs=[out, out],
        scratch_shapes=[
            pltpu.VMEM(weight.shape, jnp.float32), pltpu.SemaphoreType.DMA((FINAL + 1,)),
        ],
        compiler_params=pltpu.CompilerParams(vmem_limit_bytes=16 * 2**20),
        name="finish",
    )(weight, back, mom)


def solution(mesh):
    cols = mesh.shape["cols"]

    def on_device(grad_stack, moment_stack, weight_stack):
        back, new_momentum = exchange_and_iterate(grad_stack, moment_stack, cols)
        return tuple(finish(weight_stack, back, new_momentum))

    placed = P(None, "rows", "cols")
    return jax.shard_map(
        on_device,
        mesh=mesh,
        in_specs=(placed, placed, placed),
        out_specs=(placed, placed),
        check_vma=False,
    )
```
